32 devices in a mesh: gx: 4 (over z), yz: 8 (over y, x, core).
Axes of the slice: x: 2, y: 2, z: 4, core: 2. Of those that a mesh axis runs over, the one named last changes fastest.
Arguments:
- brick_ids: int32 [4096, 1], P(('gx', 'yz')), may hold values from 0 to 31; in each aligned block of 128 rows (0 to 127, 128 to 255, ...) at most 4 rows name the same one
- voxel_offset: int32 [4096, 256], P(('gx', 'yz')), may hold values from 0 to 4095
- fractions: float32 [4096, 3, 256], P(('gx', 'yz')), may hold values from 0 to 1
- normals: float32 [4096, 3, 256], P(('gx', 'yz')), may hold values from -6 to 6
- point_weight: float32 [4096, 256], P(('gx', 'yz')), may hold values from 0.1 to 10
- tile_count: int32 [32], P(('gx', 'yz')), may hold values from 96 to 128, as said below
Outputs:
- rhs: float32 [16, 64, 128], P('gx', 'yz')
- screen: float32 [16, 64, 128], P('gx', 'yz')
The draws below stay inside these ranges and needn't reach their ends.
Inputs may be any that keep to these rules, and one draw needn't show every extreme that they name: `brick_ids`: brick b belongs to index b // 8 of gx and b % 8 of yz. Among the 128 tile slots of one device no brick is named more than 4 times. `tile_count`: some device has all its slots valid in every draw.
All inputs are finite; a program needn't handle non-finite values.
Results may differ from the reference program's by a relative error of at most 0.0039.
Values sent between devices are 32-bit elements; how exact they have to be, the bound alone decides.
A program may use at most 64 MiB of HBM per device.

```python
import math
import jax
import jax.numpy as jnp
import numpy as np
from jax import lax

BX = 4
BY = 8
BZ = 128
TILE = 256
TILES_DEV = 128
CAP = 4
TILES = 4096
NX = 16
NY = 64
NZ = 128
N_YZ = 8
DEVICES = 32


def draw_tile_count(key, part):
    first = jax.random.fold_in(key, 11)
    second = jax.random.fold_in(key, 23)
    counts = jax.random.randint(first, (DEVICES,), max(1, 3 * TILES_DEV // 4), TILES_DEV + 1)
    filled = jax.random.randint(second, (), 0, DEVICES)
    return counts.at[filled].set(TILES_DEV).astype(jnp.int32)


def place_ends(entries, stream_key, least, high):
    longest = entries.shape.index(max(entries.shape))
    spots = []
    for shift in (0, 1):
        where = [jax.random.randint(jax.random.fold_in(stream_key, axis), (), 0, length) for axis, length in enumerate(entries.shape)]
        where[longest] = (where[longest] + shift) % entries.shape[longest]
        spots.append(tuple(where))
    return entries.at[spots[0]].set(least).at[spots[1]].set(high)


def level_of(rng, shape, cuts, low, top_value):
    factor_of = 1.0
    for dim, blocks in cuts:
        draws = jax.random.uniform(jax.random.fold_in(jax.random.fold_in(rng, 6), dim), (blocks,), jnp.float32, low / len(cuts), top_value / len(cuts))
        factor_of = factor_of * jnp.repeat(jnp.exp(draws), shape[dim] // blocks).reshape((-1,) + (1,) * (len(shape) - 1 - dim))
    return factor_of


def deal_out(key, own, number, rows, count, top, reach, slope):
    sequence = jax.random.permutation(key, count)
    crowded, usual = shares(count, rows * top, reach, slope, True), shares(count, rows * top, reach, slope, False)
    places = jnp.arange(count)

    def named(tallies, turn):
        used = int((tallies > 0).sum())
        fixed = max(1, used // 4)
        shifted = fixed + (places - fixed + turn * (used - fixed)) % max(1, count - fixed)
        return jnp.zeros((count,), jnp.int32).at[sequence[jnp.where(places < fixed, places, shifted)]].set(jnp.asarray(tallies, jnp.int32))

    tallies = jnp.where(number % 4 == 0, named(crowded, number // 4), named(usual, number - number // 4 - 1))
    mixed = jax.random.permutation(jax.random.fold_in(own, 3), count)
    donor, sink = mixed[0:count // 2 * 2:2], mixed[1:count // 2 * 2:2]
    room = jnp.minimum(tallies[donor] - 1, reach - tallies[sink]) // 2
    room = jnp.where((donor == sequence[0]) | (sink == sequence[0]) | (tallies[sink] == 0), 0, jnp.maximum(room, 0))
    shifted = jax.random.randint(jax.random.fold_in(own, 4), (count // 2,), 0, 1 << 20) % (room + 1)
    tallies = tallies.at[donor].add(-shifted).at[sink].add(shifted)
    labels = jnp.searchsorted(jnp.cumsum(tallies), jnp.arange(rows * top), side="right").astype(jnp.int32)
    grid = labels.reshape(top, rows).T
    grid = grid[jax.random.permutation(jax.random.fold_in(own, 1), rows)]
    turn = jax.random.randint(jax.random.fold_in(own, 2), (rows, 1), 0, top)
    return jnp.take_along_axis(grid, (jnp.arange(top)[None, :] + turn) % top, axis=1)


def shares(amount, total, bound, skew, full):
    weights = [(1 << 20) // math.isqrt(standing ** skew) + 1 for standing in range(1, amount + 1)]
    largest = bound if full else min(bound, max(-(-total // amount), total * weights[0] // sum(weights)))
    least = 1 if total - largest >= amount - 1 else 0
    given, spare = [largest] + [least] * (amount - 1), total - largest - least * (amount - 1)
    while spare > 0:
        movable = [i for i in range(1, amount) if given[i] < largest] or [i for i in range(1, amount) if given[i] < bound]
        whole, budget = sum([weights[i] for i in movable]), spare
        for i in movable:
            more = min(bound - given[i], max(1, budget * weights[i] // whole), spare)
            given[i] = given[i] + more
            spare = spare - more
    return np.array(given)


def bell_draw(rng, shape, scale, most, cuts=(), kind=jnp.bfloat16):
    result = jax.random.normal(rng, shape, jnp.float32) * scale
    if len(cuts) > 0:
        result = level_of(rng, shape, cuts, -0.22, 0.18) * result
    return jnp.clip(result, min=-most, max=most).astype(kind)


def setup_inputs(seed: int = 0) -> dict:
    arg_keys = jax.random.split(jax.random.key(seed), 7)
    brick_ids_keys = jax.random.split(jax.random.fold_in(arg_keys[0], 1), TILES // TILES_DEV)
    brick_ids_turns = jax.random.permutation(jax.random.fold_in(arg_keys[0], 3), TILES // TILES_DEV)
    brick_ids = jax.vmap(lambda own, number: deal_out(jax.random.fold_in(arg_keys[0], 2), own, number, TILES_DEV, DEVICES, 1, CAP, 2))(brick_ids_keys, brick_ids_turns).reshape((TILES, 1))
    voxel_offset = place_ends(jax.random.randint(arg_keys[1], (TILES, TILE), 0, BX * BY * BZ), jax.random.fold_in(arg_keys[1], 1), 0, (BX * BY * BZ) - 1).astype(jnp.int32)
    fractions = jnp.clip(1.0 * jax.random.uniform(arg_keys[2], (TILES, 3, TILE), jnp.float32) ** level_of(arg_keys[2], (TILES, 3, TILE), ((0, 32),), -0.2, 0.2), 0.0, 1.0)
    normals = bell_draw(arg_keys[3], (TILES, 3, TILE), 1.0, 6.0, ((0, 32),), jnp.float32)
    point_weight = jnp.clip(jnp.exp(math.log(10.0) - 4.6051702 * jax.random.uniform(arg_keys[4], (TILES, TILE), jnp.float32) ** level_of(arg_keys[4], (TILES, TILE), ((0, 32),), -0.2, 0.2)), 0.1, 10.0)
    tile_count = draw_tile_count(jax.random.fold_in(arg_keys[6], 71), 0)
    return dict(brick_ids=brick_ids, voxel_offset=voxel_offset, fractions=fractions, normals=normals, point_weight=point_weight, tile_count=tile_count)


def spline(frac):
    weights = jnp.stack([0.5 * (1.0 - frac) ** 2, 0.75 - (frac - 0.5) ** 2, 0.5 * frac * frac])
    slopes = jnp.stack([frac - 1.0, 1.0 - 2.0 * frac, frac])
    return weights, slopes


def rounded(value):
    return value.astype(jnp.bfloat16).astype(jnp.float32)


def reference(brick_ids, voxel_offset, fractions, normals, point_weight, tile_count):
    pad_y = NY + 2
    pad_z = NZ + 2
    total = (NX + 2) * pad_y * pad_z
    dest_all = brick_ids[:, 0].reshape(DEVICES, TILES_DEV)
    off_all = voxel_offset.reshape(DEVICES, TILES_DEV, TILE)
    frac_all = fractions.reshape(DEVICES, TILES_DEV, 3, TILE)
    norm_all = normals.reshape(DEVICES, TILES_DEV, 3, TILE)
    weight_all = point_weight.reshape(DEVICES, TILES_DEV, TILE)
    stencil = jnp.arange(3, dtype=jnp.int32)

    def step(carry, items):
        rhs_flat, screen_flat = carry
        dest, offset, frac, normal, weight, count = items
        valid = (jnp.arange(TILES_DEV, dtype=jnp.int32) < count).astype(jnp.float32)[:, None]
        normal = normal * valid[:, None, :]
        weight = weight * valid
        cell_x = offset // (BY * BZ)
        cell_y = (offset // BZ) % BY
        cell_z = offset % BZ
        base_x = (dest // N_YZ)[:, None] * BX + cell_x
        base_y = (dest % N_YZ)[:, None] * BY + cell_y
        wx, gx = spline(frac[:, 0])
        wy, gy = spline(frac[:, 1])
        wz, gz = spline(frac[:, 2])
        nx = normal[:, 0]
        ny = normal[:, 1]
        nz = normal[:, 2]
        a12 = rounded(nx[None, None] * gx[:, None] * wy[None, :] + ny[None, None] * wx[:, None] * gy[None, :])
        a3 = rounded(nz[None, None] * wx[:, None] * wy[None, :])
        a_s = rounded(weight[None, None] * wx[:, None] * wy[None, :])
        zb = rounded(wz)
        zd = rounded(gz)
        rhs_terms = a12[:, :, None] * zb[None, None] + a3[:, :, None] * zd[None, None]
        screen_terms = a_s[:, :, None] * zb[None, None]
        index = ((base_x[None, None, None] + stencil[:, None, None, None, None]) * pad_y
                 + base_y[None, None, None] + stencil[None, :, None, None, None]) * pad_z \
            + cell_z[None, None, None] + stencil[None, None, :, None, None]
        index = index.astype(jnp.int32).ravel()
        rhs_flat = rhs_flat.at[index].add(rhs_terms.ravel())
        screen_flat = screen_flat.at[index].add(screen_terms.ravel())
        return (rhs_flat, screen_flat), None

    start = (jnp.zeros((total,), jnp.float32), jnp.zeros((total,), jnp.float32))
    (rhs_flat, screen_flat), _ = lax.scan(step, start, (dest_all, off_all, frac_all, norm_all, weight_all, tile_count))
    rhs = rhs_flat.reshape(NX + 2, pad_y, pad_z)[1:-1, 1:-1, 1:-1]
    screen = screen_flat.reshape(NX + 2, pad_y, pad_z)[1:-1, 1:-1, 1:-1]
    return (rhs, screen)
```

```python
import functools

import jax
import jax.numpy as jnp
from jax import lax
from jax.experimental import pallas as pl
from jax.experimental.pallas import tpu as pltpu
from jax.sharding import PartitionSpec as P

BX = 4
BY = 8
BZ = 128
MESH = pl.DeviceIdType.MESH
HALO_X = BX + 2
ROWS_Y = 2 * BY
X_CH = 4 * HALO_X
CHANNELS = X_CH + 14


def spline(frac):
    weights = [0.5 * (1.0 - frac) ** 2, 0.75 - (frac - 0.5) ** 2, 0.5 * frac * frac]
    slopes = [frac - 1.0, 1.0 - 2.0 * frac, frac]
    return (weights, slopes)


def pick(masks, values):
    out = jnp.zeros_like(values[0])
    for mask, value in zip(masks, values):
        out = jnp.where(mask, value, out)
    return out


def prepare(rows, off_ref, frac_ref, norm_ref, weight_ref, chan):
    offset = off_ref[rows, :]
    cell_x = offset // (BY * BZ)
    cell_y = (offset // BZ) % BY
    cell_z = offset % BZ
    wx, gx = spline(frac_ref[0, rows, :])
    nx, ny, nz = norm_ref[0, rows, :], norm_ref[1, rows, :], norm_ref[2, rows, :]
    weight = weight_ref[rows, :]
    at = [cell_x == m for m in range(BX)]
    sources = ([nx * v for v in gx], [ny * v for v in wx], [nz * v for v in wx], [weight * v for v in wx])
    for i in range(HALO_X):
        for n, values in enumerate(sources):
            shifts = [k for k in range(3) if 0 <= i - k < BX]
            chan[4 * i + n, rows, :] = pick([at[i - k] for k in shifts], [values[k] for k in shifts])
    wy, gy = spline(frac_ref[1, rows, :])
    wz, gz = spline(frac_ref[2, rows, :])
    rest = [cell_y.astype(jnp.float32)] + wy + gy + [cell_z.astype(jnp.float32)] + wz + gz
    for n, value in enumerate(rest):
        chan[X_CH + n, rows, :] = value


def splat_kernel(
    capacity, n_slabs, n_columns, ids_ref, count_ref, off_ref, frac_ref, norm_ref, weight_ref, out_ref,
    table, used, chan, left, left_n, z_val, z_der, grid
):
    tiles, tile_len = off_ref.shape
    bricks = n_slabs * n_columns
    slots = bricks * capacity

    def clear(q, _):
        table[q] = -1
        return 0

    def clear_used(b, _):
        used[b] = 0
        return 0

    lax.fori_loop(0, slots, clear, 0)
    lax.fori_loop(0, bricks, clear_used, 0)

    def enter(t, _):
        brick = ids_ref[t]
        place = used[brick]
        table[brick * capacity + place] = t
        used[brick] = place + 1
        return 0

    lax.fori_loop(0, count_ref[0], enter, 0)

    def prepare_rows(step, _):
        prepare(pl.ds(pl.multiple_of(step * 8, 8), 8), off_ref, frac_ref, norm_ref, weight_ref, chan)
        return 0

    lax.fori_loop(0, tiles // 8, prepare_rows, 0)
    grid[...] = jnp.zeros_like(grid)

    row_y = lax.broadcasted_iota(jnp.int32, (ROWS_Y, tile_len), 0)
    row_y = jnp.where(row_y == ROWS_Y - 1, -1, row_y).astype(jnp.float32)
    row_z = lax.broadcasted_iota(jnp.int32, (BZ, tile_len), 0).astype(jnp.float32)
    edge = lax.broadcasted_iota(jnp.int32, (HALO_X, BY, BZ), 1)

    def brick_step(b, _):
        for c in range(capacity):
            entry = table[b * capacity + c]
            live = (entry >= 0).astype(jnp.float32)
            tile = jnp.maximum(entry, 0)
            cols = pl.ds(c * tile_len, tile_len)

            def row(n):
                return chan[n, pl.ds(tile, 1), :]

            gap = row_y - row(X_CH)
            hit = [gap == k - 1.0 for k in range(3)]
            wy = pick(hit, [jnp.broadcast_to(row(X_CH + 1 + k) * live, gap.shape) for k in range(3)])
            gy = pick(hit, [jnp.broadcast_to(row(X_CH + 4 + k) * live, gap.shape) for k in range(3)])
            for i in range(HALO_X):
                band = pl.ds(i * ROWS_Y, ROWS_Y)
                low = pl.ds((HALO_X + i) * ROWS_Y, ROWS_Y)
                left[band, cols] = (row(4 * i) * wy + row(4 * i + 1) * gy).astype(jnp.bfloat16)
                left_n[band, cols] = (row(4 * i + 2) * wy).astype(jnp.bfloat16)
                left[low, cols] = (row(4 * i + 3) * wy).astype(jnp.bfloat16)
            gap = row_z - row(X_CH + 7)
            hit = [gap == k - 1.0 for k in range(3)]
            z_val[:, cols] = pick(
                hit, [jnp.broadcast_to(row(X_CH + 8 + k), gap.shape) for k in range(3)]
            ).astype(jnp.bfloat16)
            z_der[:, cols] = pick(
                hit, [jnp.broadcast_to(row(X_CH + 11 + k), gap.shape) for k in range(3)]
            ).astype(jnp.bfloat16)
        dims = (((1,), (1,)), ((), ()))
        both = lax.dot_general(left[...], z_val[...], dims, preferred_element_type=jnp.float32)
        third = lax.dot_general(left_n[...], z_der[...], dims, preferred_element_type=jnp.float32)
        half = HALO_X * ROWS_Y
        fields = (both[:half] + third, both[half:])
        slab, column = b // n_columns, b % n_columns
        above = jnp.where(column == n_columns - 1, n_columns, column + 1)
        below = jnp.where(column == 0, n_columns, column - 1)
        where_x = pl.ds(slab * BX, HALO_X)
        for f, field in enumerate(fields):
            field = field.reshape(HALO_X, ROWS_Y, BZ)
            inner, outer = field[:, :BY], field[:, BY:]
            grid[f, column, where_x] += inner
            grid[f, above, where_x] += jnp.where(edge == 0, outer, 0.0)
            grid[f, below, where_x] += jnp.where(edge == BY - 1, outer, 0.0)
        return 0

    lax.fori_loop(0, bricks, brick_step, 0)
    for f in range(2):
        for column in range(n_columns):
            out_ref[f, column] = grid[f, column, pl.ds(1, n_slabs * BX)]


def splat(capacity, n_slabs, n_columns, ids, count, off, frac, norm, weight):
    tiles, tile_len = off.shape
    bricks = n_slabs * n_columns
    points = capacity * tile_len
    vmem = pl.BlockSpec(memory_space=pltpu.VMEM)
    smem = pl.BlockSpec(memory_space=pltpu.SMEM)
    return pl.pallas_call(
        functools.partial(splat_kernel, capacity, n_slabs, n_columns),
        out_shape=jax.ShapeDtypeStruct((2, n_columns, n_slabs * BX, BY, BZ), jnp.float32),
        in_specs=[smem, smem, vmem, vmem, vmem, vmem],
        out_specs=vmem,
        scratch_shapes=[
            pltpu.SMEM((bricks * capacity,), jnp.int32),
            pltpu.SMEM((bricks,), jnp.int32),
            pltpu.VMEM((CHANNELS, tiles, tile_len), jnp.float32),
            pltpu.VMEM((2 * HALO_X * ROWS_Y, points), jnp.bfloat16),
            pltpu.VMEM((HALO_X * ROWS_Y, points), jnp.bfloat16),
            pltpu.VMEM((BZ, points), jnp.bfloat16),
            pltpu.VMEM((BZ, points), jnp.bfloat16),
            pltpu.VMEM((2, n_columns + 1, n_slabs * BX + 2, BY, BZ), jnp.float32),
        ],
        name="splat",
    )(ids, count, off, frac, norm, weight)


def plan_of(n_slabs, n_columns):
    ybits, xbits = n_columns.bit_length() - 1, n_slabs.bit_length() - 1
    y_rest, x_all = list(range(1, ybits)), [("gx", k) for k in range(xbits)]
    orders = []
    for rest in (y_rest, y_rest[::-1]):
        orders.append([("yz", 0)] * (ybits > 0) + [("yz", k) for k in rest] + x_all)
    axes = [("yz", k) for k in reversed(range(ybits))] + [("gx", k) for k in reversed(range(xbits))]
    return axes, orders


def halving_kernel(n_slabs, n_columns, in_ref, rhs_ref, screen_ref, *scratch):
    axes, orders = plan_of(n_slabs, n_columns)
    steps = len(axes)
    got = (scratch[:steps], scratch[steps : 2 * steps])
    sums = (scratch[2 * steps : 3 * steps], scratch[3 * steps : 4 * steps])
    send_sem, recv_sem = scratch[4 * steps :]
    me = {"gx": lax.axis_index("gx"), "yz": lax.axis_index("yz")}

    def bit_of(axis, k):
        return (me[axis] // (1 << k)) % 2

    def partner(axis, k):
        other = dict(me)
        other[axis] = me[axis] + (1 - 2 * bit_of(axis, k)) * (1 << k)
        return (other["gx"], other["yz"])

    barrier = pltpu.get_barrier_semaphore()
    for axis, k in axes:
        pl.semaphore_signal(barrier, inc=1, device_id=partner(axis, k), device_id_type=MESH)
    pl.semaphore_wait(barrier, steps)

    state = [(in_ref.at[f], list(axes)) for f in range(2)]
    flying = [None, None]

    def begin(f, s):
        ref, left = state[f]
        axis, k = orders[f][s]
        at = left.index((axis, k))
        mine = bit_of(axis, k)
        lead = (slice(None),) * at
        copy = pltpu.make_async_remote_copy(
            src_ref=ref.at[lead + (1 - mine,)],
            dst_ref=got[f][s],
            send_sem=send_sem.at[f, s],
            recv_sem=recv_sem.at[f, s],
            device_id=partner(axis, k),
            device_id_type=MESH,
        )
        copy.start()
        flying[f] = (copy, ref, lead + (mine,), left[:at] + left[at + 1 :])

    for f in range(2):
        begin(f, 0)
    for s in range(steps):
        for f in range(2):
            copy, ref, keep, left = flying[f]
            copy.wait()
            total = ref[keep] + got[f][s][...]
            if s == steps - 1:
                (rhs_ref, screen_ref)[f][...] = total
            else:
                sums[f][s][...] = total
                state[f] = (sums[f][s], left)
                begin(f, s + 1)


def halving(n_slabs, n_columns, field):
    axes, orders = plan_of(n_slabs, n_columns)
    steps = len(axes)
    block = (BX, BY, BZ)
    field = field.reshape((2,) + (2,) * steps + block)
    shapes = [pltpu.VMEM((2,) * (steps - 1 - s) + block, jnp.float32) for s in range(steps)]
    vmem = pl.BlockSpec(memory_space=pltpu.VMEM)
    return pl.pallas_call(
        functools.partial(halving_kernel, n_slabs, n_columns),
        out_shape=[jax.ShapeDtypeStruct(block, jnp.float32)] * 2,
        in_specs=[vmem],
        out_specs=[vmem, vmem],
        scratch_shapes=shapes * 4 + [pltpu.SemaphoreType.DMA((2, steps)), pltpu.SemaphoreType.DMA((2, steps))],
        compiler_params=pltpu.CompilerParams(collective_id=0, has_side_effects=True),
        name="halving",
    )(field)


def shards(brick_ids, voxel_offset, fractions, normals, point_weight, tile_count):
    n_slabs = lax.axis_size("gx")
    n_columns = lax.axis_size("yz")
    devices = n_slabs * n_columns
    tiles_here = brick_ids.shape[0]
    capacity = max(2, (tiles_here + devices - 1) // devices)
    field = splat(
        capacity, n_slabs, n_columns, brick_ids.reshape(tiles_here), tile_count, voxel_offset,
        jnp.transpose(fractions, (1, 0, 2)), jnp.transpose(normals, (1, 0, 2)), point_weight,
    )
    rhs, screen = halving(n_slabs, n_columns, field)
    return (rhs, screen)


def solution(mesh):
    return jax.shard_map(
        shards,
        mesh=mesh,
        in_specs=(
            P(("gx", "yz"), None),
            P(("gx", "yz"), None),
            P(("gx", "yz"), None, None),
            P(("gx", "yz"), None, None),
            P(("gx", "yz"), None),
            P(("gx", "yz")),
        ),
        out_specs=(P("gx", "yz", None), P("gx", "yz", None)),
        check_vma=False,
    )
```

```python
import functools

import jax
import jax.numpy as jnp
from jax import lax
from jax.experimental import pallas as pl
from jax.experimental.pallas import tpu as pltpu
from jax.sharding import PartitionSpec as P

BX = 4
BY = 8
BZ = 128
MESH = pl.DeviceIdType.MESH
HALO_X = BX + 2
ROWS_Y = 2 * BY
X_CH = 4 * HALO_X
CHANNELS = X_CH + 14


def spline(frac):
    weights = [0.5 * (1.0 - frac) ** 2, 0.75 - (frac - 0.5) ** 2, 0.5 * frac * frac]
    slopes = [frac - 1.0, 1.0 - 2.0 * frac, frac]
    return (weights, slopes)


def pick(masks, values):
    out = jnp.zeros_like(values[0])
    for mask, value in zip(masks, values):
        out = jnp.where(mask, value, out)
    return out


def prepare(rows, off_ref, frac_ref, norm_ref, weight_ref, chan):
    offset = off_ref[rows, :]
    cell_x = offset // (BY * BZ)
    cell_y = (offset // BZ) % BY
    cell_z = offset % BZ
    wx, gx = spline(frac_ref[0, rows, :])
    nx, ny, nz = norm_ref[0, rows, :], norm_ref[1, rows, :], norm_ref[2, rows, :]
    weight = weight_ref[rows, :]
    at = [cell_x == m for m in range(BX)]
    sources = ([nx * v for v in gx], [ny * v for v in wx], [nz * v for v in wx], [weight * v for v in wx])
    for i in range(HALO_X):
        for n, values in enumerate(sources):
            shifts = [k for k in range(3) if 0 <= i - k < BX]
            chan[4 * i + n, rows, :] = pick([at[i - k] for k in shifts], [values[k] for k in shifts])
    wy, gy = spline(frac_ref[1, rows, :])
    wz, gz = spline(frac_ref[2, rows, :])
    rest = [cell_y.astype(jnp.float32)] + wy + gy + [cell_z.astype(jnp.float32)] + wz + gz
    for n, value in enumerate(rest):
        chan[X_CH + n, rows, :] = value


def stage_orders(n_columns):
    bits = n_columns.bit_length() - 1
    rest = list(range(1, bits))
    first = [0] if bits else []
    return [first + rest, first + rest[::-1]]


def fused_kernel(
    capacity, n_slabs, n_columns, table_ref, off_ref, frac_ref, norm_ref, weight_ref, rhs_ref, screen_ref,
    chan, left_a, left_b, third_a, third_b, val_a, val_b, der_a, der_b, grid, done, z_main, z_low, z_high,
    send_sem, recv_sem, send_z, recv_z, *stages
):
    tiles, tile_len = off_ref.shape
    orders = stage_orders(n_columns)
    steps = len(orders[0])
    starts = stages[:2]
    got = (stages[2 : 2 + steps], stages[2 + steps : 2 + 2 * steps])
    sums = (stages[2 + 2 * steps : 1 + 3 * steps], stages[1 + 3 * steps : 4 * steps])
    me_x, me_y = lax.axis_index("gx"), lax.axis_index("yz")
    bufs = ((left_a, third_a, val_a, der_a), (left_b, third_b, val_b, der_b))

    def slab_of(step):
        return lax.rem(me_x + 1 + step, n_slabs)

    def bit_of(k):
        return lax.rem(me_y // (1 << k), 2)

    def partner(k):
        return (me_x, me_y + (1 - 2 * bit_of(k)) * (1 << k))

    barrier = pltpu.get_barrier_semaphore()
    for k in range(steps):
        pl.semaphore_signal(barrier, inc=1, device_id=partner(k), device_id_type=MESH)
    for hop in range(1, n_slabs):
        other = (lax.rem(me_x + hop, n_slabs), me_y)
        pl.semaphore_signal(barrier, inc=1, device_id=other, device_id_type=MESH)

    def prepare_rows(step, _):
        prepare(pl.ds(pl.multiple_of(step * 8, 8), 8), off_ref, frac_ref, norm_ref, weight_ref, chan)
        return 0

    lax.fori_loop(0, tiles // 8, prepare_rows, 0)
    grid[...] = jnp.zeros_like(grid)

    row_y = lax.broadcasted_iota(jnp.int32, (ROWS_Y, tile_len), 0)
    row_y = jnp.where(row_y == ROWS_Y - 1, -1, row_y).astype(jnp.float32)
    pack = 16
    row_z = lax.broadcasted_iota(jnp.int32, (pack, tile_len), 0).astype(jnp.float32)
    edge = lax.broadcasted_iota(jnp.int32, (HALO_X, BY, BZ), 1)
    last = n_slabs * n_columns - 1

    def build(g, buf):
        left, third, val, der = buf
        brick = slab_of(g // n_columns) * n_columns + lax.rem(g, n_columns)
        for c in range(capacity):
            entry = table_ref[brick * capacity + c]
            live = (entry >= 0).astype(jnp.float32)
            tile = jnp.maximum(entry, 0)
            cols = pl.ds(c * tile_len, tile_len)

            def row(n):
                return chan[n, pl.ds(tile, 1), :]

            gap = row_y - row(X_CH)
            hit = [gap == k - 1.0 for k in range(3)]
            wy = pick(hit, [jnp.broadcast_to(row(X_CH + 1 + k) * live, gap.shape) for k in range(3)])
            gy = pick(hit, [jnp.broadcast_to(row(X_CH + 4 + k) * live, gap.shape) for k in range(3)])
            for i in range(HALO_X):
                band = pl.ds(i * ROWS_Y, ROWS_Y)
                low = pl.ds((HALO_X + i) * ROWS_Y, ROWS_Y)
                left[band, cols] = (row(4 * i) * wy + row(4 * i + 1) * gy).astype(jnp.bfloat16)
                third[band, cols] = (row(4 * i + 2) * wy).astype(jnp.bfloat16)
                left[low, cols] = (row(4 * i + 3) * wy).astype(jnp.bfloat16)
            wide = [
                jnp.broadcast_to(row(X_CH + 8 + k), row_z.shape).astype(jnp.bfloat16) for k in range(6)
            ]
            base = (row_z - row(X_CH + 7)).astype(jnp.bfloat16)
            for group in range(BZ // pack):
                rows = pl.ds(group * pack, pack)
                hit = [base == jnp.bfloat16(k - 1.0 - group * pack) for k in range(3)]
                val[rows, cols] = pick(hit, wide[:3])
                der[rows, cols] = pick(hit, wide[3:])

    def multiply(g, buf):
        left, third, val, der = buf
        dims = (((1,), (1,)), ((), ()))
        both = lax.dot_general(left[...], val[...], dims, preferred_element_type=jnp.float32)
        part = lax.dot_general(third[...], der[...], dims, preferred_element_type=jnp.float32)
        half = HALO_X * ROWS_Y
        column = lax.rem(g, n_columns)
        above = jnp.where(column == n_columns - 1, n_columns, column + 1)
        below = jnp.where(column == 0, n_columns, column - 1)
        for f, field in enumerate((both[:half] + part, both[half:])):
            field = field.reshape(HALO_X, ROWS_Y, BZ)
            inner, outer = field[:, :BY], field[:, BY:]
            grid[f, column] += inner
            grid[f, above] += jnp.where(edge == 0, outer, 0.0)
            grid[f, below] += jnp.where(edge == BY - 1, outer, 0.0)

    def stage_refs(f, s, j):
        ref = (starts[f] if s == 0 else sums[f][s - 1]).at[j]
        alive = [k for k in reversed(range(steps)) if k not in orders[f][:s]]
        k = orders[f][s]
        lead = (slice(None),) * alive.index(k)
        return ref, lead, k

    def stage_copy(f, s, j):
        ref, lead, k = stage_refs(f, s, j)
        return pltpu.make_async_remote_copy(
            src_ref=ref.at[lead + (1 - bit_of(k),)],
            dst_ref=got[f][s].at[j],
            send_sem=send_sem.at[f, s, j],
            recv_sem=recv_sem.at[f, s, j],
            device_id=partner(k),
            device_id_type=MESH,
        )

    def cross_copy(kind, j):
        source = (done.at[j, :, pl.ds(1, BX)], done.at[j, :, pl.ds(0, 1)], done.at[j, :, pl.ds(BX + 1, 1)])[kind]
        target = (z_main, z_low, z_high)[kind].at[j]
        owner = lax.rem(me_x + (1, n_slabs, 2)[kind] + j, n_slabs)
        return pltpu.make_async_remote_copy(
            src_ref=source,
            dst_ref=target,
            send_sem=send_z.at[kind, j],
            recv_sem=recv_z.at[kind, j],
            device_id=(owner, me_y),
            device_id_type=MESH,
        )

    at_home = (n_slabs - 1, 0, n_slabs - 2)

    def cross_start(kind, j):
        if isinstance(j, int):
            if j != at_home[kind]:
                cross_copy(kind, j).start()
        else:
            @pl.when(j != at_home[kind])
            def _():
                cross_copy(kind, j).start()

    def event(s, j):
        for f in range(2):
            stage_copy(f, s - 1, j).wait()
            ref, lead, k = stage_refs(f, s - 1, j)
            total = ref[lead + (bit_of(k),)] + got[f][s - 1][j]
            if s == steps:
                done[j, f] = total
            else:
                sums[f][s - 1][j] = total
                stage_copy(f, s, j).start()
        if s == steps:
            for kind in range(3):
                cross_start(kind, j)

    build(0, bufs[0])
    pl.semaphore_wait(barrier, steps + n_slabs - 1)
    pairs = n_columns // 4

    def half_step(h, _):
        step, half = h // 2, lax.rem(h, 2)

        def pair(p, _):
            g = (h * pairs + p) * 2
            build(g + 1, bufs[1])
            multiply(g, bufs[0])
            build(jnp.minimum(g + 2, last), bufs[0])
            multiply(g + 1, bufs[1])
            return 0

        lax.fori_loop(0, pairs, pair, 0)

        @pl.when(half == 1)
        def _():
            for f in range(2):
                for column in range(n_columns):
                    bits = tuple((column >> k) & 1 for k in reversed(range(steps)))
                    starts[f][(step,) + bits] = grid[f, column]
                stage_copy(f, 0, step).start()
            grid[...] = jnp.zeros_like(grid)

        for s in range(1, steps + 1):
            @pl.when((half == 0) & (step >= s))
            def _():
                event(s, step - s)

        return 0

    lax.fori_loop(0, 2 * n_slabs, half_step, 0)
    for r in range(1, steps + 1):
        for s in range(r, steps + 1):
            if n_slabs - 1 - (s - r) >= 0:
                event(s, n_slabs - 1 - (s - r))

    main = [done[n_slabs - 1, f, pl.ds(1, BX)] for f in range(2)]
    low = [done[0, f, 0] for f in range(2)]
    high = [done[n_slabs - 2, f, BX + 1] for f in range(2)]
    for j in range(n_slabs):
        for kind in range(3):
            if j != at_home[kind]:
                cross_copy(kind, j).wait()
                for f in range(2):
                    if kind == 0:
                        main[f] = main[f] + z_main[j, f]
                    elif kind == 1:
                        low[f] = low[f] + z_low[j, f, 0]
                    else:
                        high[f] = high[f] + z_high[j, f, 0]
    for f, out in enumerate((rhs_ref, screen_ref)):
        out[...] = main[f]
        out[BX - 1] += jnp.where(me_x < n_slabs - 1, low[f], 0.0)
        out[0] += jnp.where(me_x > 0, high[f], 0.0)


def fused(capacity, n_slabs, n_columns, table, off, frac, norm, weight):
    tiles, tile_len = off.shape
    points = capacity * tile_len
    steps = n_columns.bit_length() - 1
    block = (HALO_X, BY, BZ)
    vmem = pl.BlockSpec(memory_space=pltpu.VMEM)
    smem = pl.BlockSpec(memory_space=pltpu.SMEM)

    def stage(s):
        return pltpu.VMEM((n_slabs,) + (2,) * (steps - s) + block, jnp.float32)

    got = [stage(s + 1) for s in range(steps)]
    sums = [stage(s + 1) for s in range(steps - 1)]
    return pl.pallas_call(
        functools.partial(fused_kernel, capacity, n_slabs, n_columns),
        out_shape=[jax.ShapeDtypeStruct((BX, BY, BZ), jnp.float32)] * 2,
        in_specs=[smem, vmem, vmem, vmem, vmem],
        out_specs=[vmem, vmem],
        scratch_shapes=[pltpu.VMEM((CHANNELS, tiles, tile_len), jnp.float32)]
        + [pltpu.VMEM((2 * HALO_X * ROWS_Y, points), jnp.bfloat16)] * 2
        + [pltpu.VMEM((HALO_X * ROWS_Y, points), jnp.bfloat16)] * 2
        + [pltpu.VMEM((BZ, points), jnp.bfloat16)] * 4
        + [
            pltpu.VMEM((2, n_columns + 1) + block, jnp.float32),
            pltpu.VMEM((n_slabs, 2) + block, jnp.float32),
            pltpu.VMEM((n_slabs, 2, BX, BY, BZ), jnp.float32),
            pltpu.VMEM((n_slabs, 2, 1, BY, BZ), jnp.float32),
            pltpu.VMEM((n_slabs, 2, 1, BY, BZ), jnp.float32),
            pltpu.SemaphoreType.DMA((2, steps, n_slabs)),
            pltpu.SemaphoreType.DMA((2, steps, n_slabs)),
            pltpu.SemaphoreType.DMA((3, n_slabs)),
            pltpu.SemaphoreType.DMA((3, n_slabs)),
        ]
        + [stage(0)] * 2 + got * 2 + sums * 2,
        compiler_params=pltpu.CompilerParams(collective_id=0, has_side_effects=True),
        name="fused",
    )(table, off, frac, norm, weight)


def brick_table(capacity, bricks, dest, count):
    tiles = dest.shape[0]
    order = jnp.arange(tiles, dtype=jnp.int32)
    valid = order < count
    earlier = (dest[:, None] == dest[None, :]) & valid[None, :] & (order[None, :] < order[:, None])
    rank = jnp.sum(earlier.astype(jnp.int32), axis=1)
    slot = jnp.where(valid, dest * capacity + rank, -1)
    slots = jnp.arange(bricks * capacity, dtype=jnp.int32)
    found = jnp.where(slots[:, None] == slot[None, :], order[None, :], -1)
    return jnp.max(found, axis=1)


def shards(brick_ids, voxel_offset, fractions, normals, point_weight, tile_count):
    n_slabs = lax.axis_size("gx")
    n_columns = lax.axis_size("yz")
    devices = n_slabs * n_columns
    tiles_here = brick_ids.shape[0]
    capacity = max(2, (tiles_here + devices - 1) // devices)
    table = brick_table(capacity, devices, brick_ids.reshape(tiles_here), tile_count[0])
    rhs, screen = fused(
        capacity, n_slabs, n_columns, table, voxel_offset,
        jnp.transpose(fractions, (1, 0, 2)), jnp.transpose(normals, (1, 0, 2)), point_weight,
    )
    return (rhs, screen)


def solution(mesh):
    return jax.shard_map(
        shards,
        mesh=mesh,
        in_specs=(
            P(("gx", "yz"), None),
            P(("gx", "yz"), None),
            P(("gx", "yz"), None, None),
            P(("gx", "yz"), None, None),
            P(("gx", "yz"), None),
            P(("gx", "yz")),
        ),
        out_specs=(P("gx", "yz", None), P("gx", "yz", None)),
        check_vma=False,
    )
```

```python
import functools

import jax
import jax.numpy as jnp
from jax import lax
from jax.experimental import pallas as pl
from jax.experimental.pallas import tpu as pltpu
from jax.sharding import PartitionSpec as P

BX = 4
BY = 8
BZ = 128
MESH = pl.DeviceIdType.MESH
HALO_X = BX + 2
ROWS_Y = 2 * BY
X_CH = 4 * HALO_X
CHANNELS = X_CH + 19
PACK = 16


def spline(frac):
    weights = [0.5 * (1.0 - frac) ** 2, 0.75 - (frac - 0.5) ** 2, 0.5 * frac * frac]
    slopes = [frac - 1.0, 1.0 - 2.0 * frac, frac]
    return (weights, slopes)


def pick(masks, values):
    out = jnp.zeros_like(values[0])
    for mask, value in zip(masks, values):
        out = jnp.where(mask, value, out)
    return out


def prepare(rows, off_ref, frac_ref, norm_ref, weight_ref, chan):
    parts, lanes = chan.shape[1], chan.shape[3]

    def keep(n, value):
        for part in range(parts):
            chan[n, part, rows, :] = value[:, part * lanes : (part + 1) * lanes]

    offset = off_ref[rows, :]
    z_bits, y_bits = BZ.bit_length() - 1, BY.bit_length() - 1
    cell_x = offset >> (z_bits + y_bits)
    cell_y = (offset >> z_bits) & (BY - 1)
    cell_z = offset & (BZ - 1)
    wx, gx = spline(frac_ref[0, rows, :])
    nx, ny, nz = norm_ref[0, rows, :], norm_ref[1, rows, :], norm_ref[2, rows, :]
    weight = weight_ref[rows, :]
    at = [cell_x == m for m in range(BX)]
    sources = ([nx * v for v in gx], [ny * v for v in wx], [nz * v for v in wx], [weight * v for v in wx])
    for i in range(HALO_X):
        for n, values in enumerate(sources):
            shifts = [k for k in range(3) if 0 <= i - k < BX]
            keep(4 * i + n, pick([at[i - k] for k in shifts], [values[k] for k in shifts]))
    wy, gy = spline(frac_ref[1, rows, :])
    wz, gz = spline(frac_ref[2, rows, :])
    near = [cell_z + (k - 1) for k in range(3)]
    shift = PACK.bit_length() - 1
    rest = [cell_y.astype(jnp.float32)] + wy + gy + wz + gz
    rest += [(z & (PACK - 1)).astype(jnp.float32) for z in near] + [(z >> shift).astype(jnp.float32) for z in near]
    for n, value in enumerate(rest):
        keep(X_CH + n, value)


def stage_orders(n_columns):
    bits = n_columns.bit_length() - 1
    rest = list(range(1, bits))
    first = [0] if bits else []
    return [first + rest, first + rest[::-1]]


def fused_kernel(
    capacity, n_slabs, n_columns, table_ref, off_ref, frac_ref, norm_ref, weight_ref, rhs_ref, screen_ref,
    chan, left_a, left_b, third_a, third_b, val_a, val_b, der_a, der_b, grid, done, z_main, z_low, z_high,
    send_sem, recv_sem, send_z, recv_z, *stages
):
    tiles, tile_len = off_ref.shape
    orders = stage_orders(n_columns)
    steps = len(orders[0])
    starts = stages[:2]
    got = (stages[2 : 2 + steps], stages[2 + steps : 2 + 2 * steps])
    sums = (stages[2 + 2 * steps : 1 + 3 * steps], stages[1 + 3 * steps : 4 * steps])
    me_x, me_y = lax.axis_index("gx"), lax.axis_index("yz")
    bufs = ((left_a, third_a, val_a, der_a), (left_b, third_b, val_b, der_b))

    def slab_of(step):
        return lax.rem(me_x + 1 + step, n_slabs)

    def bit_of(k):
        return lax.rem(me_y // (1 << k), 2)

    def partner(k):
        return (me_x, me_y + (1 - 2 * bit_of(k)) * (1 << k))

    barrier = pltpu.get_barrier_semaphore()
    for k in range(steps):
        pl.semaphore_signal(barrier, inc=1, device_id=partner(k), device_id_type=MESH)
    for hop in range(1, n_slabs):
        other = (lax.rem(me_x + hop, n_slabs), me_y)
        pl.semaphore_signal(barrier, inc=1, device_id=other, device_id_type=MESH)

    def prepare_rows(step, _):
        prepare(pl.ds(pl.multiple_of(step * 8, 8), 8), off_ref, frac_ref, norm_ref, weight_ref, chan)
        return 0

    lax.fori_loop(0, tiles // 8, prepare_rows, 0)
    grid[...] = jnp.zeros_like(grid)

    lanes = tile_len
    row_y = lax.broadcasted_iota(jnp.int32, (ROWS_Y, lanes), 0)
    row_y = jnp.where(row_y == ROWS_Y - 1, -1, row_y).astype(jnp.float32)
    row_z = lax.broadcasted_iota(jnp.int32, (PACK, lanes), 0).astype(jnp.float32)
    edge = lax.broadcasted_iota(jnp.int32, (HALO_X, BY, BZ), 1)
    last = n_slabs * n_columns - 1

    def build(g, buf):
        left, third, val, der = buf
        brick = slab_of(g // n_columns) * n_columns + lax.rem(g, n_columns)
        for c in range(capacity):
            entry = table_ref[brick * capacity + c]
            away = jnp.where(entry >= 0, 0.0, 1.0) * (4.0 * BY)
            tile = jnp.maximum(entry, 0)
            for part in range(tile_len // lanes):
                cols = pl.ds(c * tile_len + part * lanes, lanes)

                def row(n):
                    return chan[n, part, pl.ds(tile, 1), :]

                gap = row_y - (row(X_CH) + away)
                hit = [gap == k - 1.0 for k in range(3)]
                wy = pick(hit, [jnp.broadcast_to(row(X_CH + 1 + k), gap.shape) for k in range(3)])
                gy = pick(hit, [jnp.broadcast_to(row(X_CH + 4 + k), gap.shape) for k in range(3)])
                for i in range(HALO_X):
                    band = pl.ds(i * ROWS_Y, ROWS_Y)
                    low = pl.ds((HALO_X + i) * ROWS_Y, ROWS_Y)
                    left[band, cols] = (row(4 * i) * wy + row(4 * i + 1) * gy).astype(jnp.bfloat16)
                    third[band, cols] = (row(4 * i + 2) * wy).astype(jnp.bfloat16)
                    left[low, cols] = (row(4 * i + 3) * wy).astype(jnp.bfloat16)
                hit = [row_z == row(X_CH + 13 + k) for k in range(3)]

                def spread(n, other):
                    for k in range(3):
                        other = jnp.where(hit[k], jnp.broadcast_to(row(X_CH + n + k), row_z.shape), other)
                    return other.astype(jnp.bfloat16)

                value = spread(7, jnp.zeros_like(row_z))
                slope = spread(10, jnp.zeros_like(row_z))
                home = spread(16, jnp.full_like(row_z, -1.0))
                zero = jnp.zeros_like(value)
                for group in range(BZ // PACK):
                    rows = pl.ds(group * PACK, PACK)
                    here = home == jnp.bfloat16(group)
                    val[rows, cols] = jnp.where(here, value, zero)
                    der[rows, cols] = jnp.where(here, slope, zero)

    def multiply(g, buf):
        left, third, val, der = buf
        dims = (((1,), (1,)), ((), ()))
        both = lax.dot_general(left[...], val[...], dims, preferred_element_type=jnp.float32)
        part = lax.dot_general(third[...], der[...], dims, preferred_element_type=jnp.float32)
        half = HALO_X * ROWS_Y
        column = lax.rem(g, n_columns)
        above = jnp.where(column == n_columns - 1, n_columns, column + 1)
        below = jnp.where(column == 0, n_columns, column - 1)
        for f, field in enumerate((both[:half] + part, both[half:])):
            field = field.reshape(HALO_X, ROWS_Y, BZ)
            inner, outer = field[:, :BY], field[:, BY:]
            grid[f, column] += inner
            grid[f, above] += jnp.where(edge == 0, outer, 0.0)
            grid[f, below] += jnp.where(edge == BY - 1, outer, 0.0)

    def stage_refs(f, s, j):
        ref = (starts[f] if s == 0 else sums[f][s - 1]).at[j]
        alive = [k for k in reversed(range(steps)) if k not in orders[f][:s]]
        k = orders[f][s]
        lead = (slice(None),) * alive.index(k)
        return ref, lead, k

    def stage_copy(f, s, j):
        ref, lead, k = stage_refs(f, s, j)
        return pltpu.make_async_remote_copy(
            src_ref=ref.at[lead + (1 - bit_of(k),)],
            dst_ref=got[f][s].at[j],
            send_sem=send_sem.at[f, s, j],
            recv_sem=recv_sem.at[f, s, j],
            device_id=partner(k),
            device_id_type=MESH,
        )

    def cross_copy(kind, j):
        source = (done.at[j, :, pl.ds(1, BX)], done.at[j, :, pl.ds(0, 1)], done.at[j, :, pl.ds(BX + 1, 1)])[kind]
        target = (z_main, z_low, z_high)[kind].at[j]
        owner = lax.rem(me_x + (1, n_slabs, 2)[kind] + j, n_slabs)
        return pltpu.make_async_remote_copy(
            src_ref=source,
            dst_ref=target,
            send_sem=send_z.at[kind, j],
            recv_sem=recv_z.at[kind, j],
            device_id=(owner, me_y),
            device_id_type=MESH,
        )

    at_home = (n_slabs - 1, 0, n_slabs - 2)

    def cross_start(kind, j):
        if isinstance(j, int):
            if j != at_home[kind]:
                cross_copy(kind, j).start()
        else:
            @pl.when(j != at_home[kind])
            def _():
                cross_copy(kind, j).start()

    def event(s, j):
        for f in range(2):
            stage_copy(f, s - 1, j).wait()
            ref, lead, k = stage_refs(f, s - 1, j)
            total = ref[lead + (bit_of(k),)] + got[f][s - 1][j]
            if s == steps:
                done[j, f] = total
            else:
                sums[f][s - 1][j] = total
                stage_copy(f, s, j).start()
        if s == steps:
            for kind in range(3):
                cross_start(kind, j)

    build(0, bufs[0])
    pl.semaphore_wait(barrier, steps + n_slabs - 1)
    pairs = n_columns // 4

    def half_step(h, _):
        step, half = h // 2, lax.rem(h, 2)

        def pair(p, _):
            g = (h * pairs + p) * 2
            build(g + 1, bufs[1])
            multiply(g, bufs[0])
            build(jnp.minimum(g + 2, last), bufs[0])
            multiply(g + 1, bufs[1])
            return 0

        lax.fori_loop(0, pairs, pair, 0)

        @pl.when(half == 1)
        def _():
            for f in range(2):
                for column in range(n_columns):
                    bits = tuple((column >> k) & 1 for k in reversed(range(steps)))
                    starts[f][(step,) + bits] = grid[f, column]
                stage_copy(f, 0, step).start()
            grid[...] = jnp.zeros_like(grid)

        for s in range(1, steps + 1):
            @pl.when((half == (0 if s == 1 else 1)) & (step >= s))
            def _():
                event(s, step - s)

        return 0

    lax.fori_loop(0, 2 * n_slabs, half_step, 0)
    for r in range(1, steps + 1):
        for s in range(r, steps + 1):
            if n_slabs - 1 - (s - r) >= 0:
                event(s, n_slabs - 1 - (s - r))

    main = [done[n_slabs - 1, f, pl.ds(1, BX)] for f in range(2)]
    low = [done[0, f, 0] for f in range(2)]
    high = [done[n_slabs - 2, f, BX + 1] for f in range(2)]
    for j in range(n_slabs):
        for kind in range(3):
            if j != at_home[kind]:
                cross_copy(kind, j).wait()
                for f in range(2):
                    if kind == 0:
                        main[f] = main[f] + z_main[j, f]
                    elif kind == 1:
                        low[f] = low[f] + z_low[j, f, 0]
                    else:
                        high[f] = high[f] + z_high[j, f, 0]
    for f, out in enumerate((rhs_ref, screen_ref)):
        out[...] = main[f]
        out[BX - 1] += jnp.where(me_x < n_slabs - 1, low[f], 0.0)
        out[0] += jnp.where(me_x > 0, high[f], 0.0)


def fused(capacity, n_slabs, n_columns, table, off, frac, norm, weight):
    tiles, tile_len = off.shape
    points = capacity * tile_len
    lanes = tile_len
    steps = n_columns.bit_length() - 1
    block = (HALO_X, BY, BZ)
    vmem = pl.BlockSpec(memory_space=pltpu.VMEM)
    smem = pl.BlockSpec(memory_space=pltpu.SMEM)

    def stage(s):
        return pltpu.VMEM((n_slabs,) + (2,) * (steps - s) + block, jnp.float32)

    got = [stage(s + 1) for s in range(steps)]
    sums = [stage(s + 1) for s in range(steps - 1)]
    return pl.pallas_call(
        functools.partial(fused_kernel, capacity, n_slabs, n_columns),
        out_shape=[jax.ShapeDtypeStruct((BX, BY, BZ), jnp.float32)] * 2,
        in_specs=[smem, vmem, vmem, vmem, vmem],
        out_specs=[vmem, vmem],
        scratch_shapes=[pltpu.VMEM((CHANNELS, tile_len // lanes, tiles, lanes), jnp.float32)]
        + [pltpu.VMEM((2 * HALO_X * ROWS_Y, points), jnp.bfloat16)] * 2
        + [pltpu.VMEM((HALO_X * ROWS_Y, points), jnp.bfloat16)] * 2
        + [pltpu.VMEM((BZ, points), jnp.bfloat16)] * 4
        + [
            pltpu.VMEM((2, n_columns + 1) + block, jnp.float32),
            pltpu.VMEM((n_slabs, 2) + block, jnp.float32),
            pltpu.VMEM((n_slabs, 2, BX, BY, BZ), jnp.float32),
            pltpu.VMEM((n_slabs, 2, 1, BY, BZ), jnp.float32),
            pltpu.VMEM((n_slabs, 2, 1, BY, BZ), jnp.float32),
            pltpu.SemaphoreType.DMA((2, steps, n_slabs)),
            pltpu.SemaphoreType.DMA((2, steps, n_slabs)),
            pltpu.SemaphoreType.DMA((3, n_slabs)),
            pltpu.SemaphoreType.DMA((3, n_slabs)),
        ]
        + [stage(0)] * 2 + got * 2 + sums * 2,
        compiler_params=pltpu.CompilerParams(collective_id=0, has_side_effects=True),
        name="fused",
    )(table, off, frac, norm, weight)


def brick_table(capacity, bricks, dest, count):
    tiles = dest.shape[0]
    order = jnp.arange(tiles, dtype=jnp.int32)
    valid = order < count
    earlier = (dest[:, None] == dest[None, :]) & valid[None, :] & (order[None, :] < order[:, None])
    rank = jnp.sum(earlier.astype(jnp.int32), axis=1)
    slot = jnp.where(valid, dest * capacity + rank, -1)
    slots = jnp.arange(bricks * capacity, dtype=jnp.int32)
    found = jnp.where(slots[:, None] == slot[None, :], order[None, :], -1)
    return jnp.max(found, axis=1)


def shards(brick_ids, voxel_offset, fractions, normals, point_weight, tile_count):
    n_slabs = lax.axis_size("gx")
    n_columns = lax.axis_size("yz")
    devices = n_slabs * n_columns
    tiles_here = brick_ids.shape[0]
    capacity = max(2, (tiles_here + devices - 1) // devices)
    table = brick_table(capacity, devices, brick_ids.reshape(tiles_here), tile_count[0])
    rhs, screen = fused(
        capacity, n_slabs, n_columns, table, voxel_offset,
        jnp.transpose(fractions, (1, 0, 2)), jnp.transpose(normals, (1, 0, 2)), point_weight,
    )
    return (rhs, screen)


def solution(mesh):
    return jax.shard_map(
        shards,
        mesh=mesh,
        in_specs=(
            P(("gx", "yz"), None),
            P(("gx", "yz"), None),
            P(("gx", "yz"), None, None),
            P(("gx", "yz"), None, None),
            P(("gx", "yz"), None),
            P(("gx", "yz")),
        ),
        out_specs=(P("gx", "yz", None), P("gx", "yz", None)),
        check_vma=False,
    )
```

```python
import functools

import jax
import jax.numpy as jnp
from jax import lax
from jax.experimental import pallas as pl
from jax.experimental.pallas import tpu as pltpu
from jax.sharding import PartitionSpec as P

BX = 4
BY = 8
BZ = 128
MESH = pl.DeviceIdType.MESH
HALO_X = BX + 2
ROWS_Y = 2 * BY
X_CH = 4 * HALO_X
CHANNELS = X_CH + 19
PACK = 16


def spline(frac):
    weights = [0.5 * (1.0 - frac) ** 2, 0.75 - (frac - 0.5) ** 2, 0.5 * frac * frac]
    slopes = [frac - 1.0, 1.0 - 2.0 * frac, frac]
    return (weights, slopes)


def pick(masks, values):
    out = jnp.zeros_like(values[0])
    for mask, value in zip(masks, values):
        out = jnp.where(mask, value, out)
    return out


def prepare(rows, off_ref, frac_ref, norm_ref, weight_ref, chan):
    parts, lanes = chan.shape[1], chan.shape[3]

    def keep(n, value):
        for part in range(parts):
            chan[n, part, rows, :] = value[:, part * lanes : (part + 1) * lanes]

    offset = off_ref[rows, :]
    z_bits, y_bits = BZ.bit_length() - 1, BY.bit_length() - 1
    cell_x = offset >> (z_bits + y_bits)
    cell_y = (offset >> z_bits) & (BY - 1)
    cell_z = offset & (BZ - 1)
    wx, gx = spline(frac_ref[0, rows, :])
    nx, ny, nz = norm_ref[0, rows, :], norm_ref[1, rows, :], norm_ref[2, rows, :]
    weight = weight_ref[rows, :]
    at = [cell_x == m for m in range(BX)]
    sources = ([nx * v for v in gx], [ny * v for v in wx], [nz * v for v in wx], [weight * v for v in wx])
    for i in range(HALO_X):
        for n, values in enumerate(sources):
            shifts = [k for k in range(3) if 0 <= i - k < BX]
            keep(4 * i + n, pick([at[i - k] for k in shifts], [values[k] for k in shifts]))
    wy, gy = spline(frac_ref[1, rows, :])
    wz, gz = spline(frac_ref[2, rows, :])
    near = [cell_z + (k - 1) for k in range(3)]
    shift = PACK.bit_length() - 1
    rest = [cell_y.astype(jnp.float32)] + wy + gy + wz + gz
    rest += [(z & (PACK - 1)).astype(jnp.float32) for z in near] + [(z >> shift).astype(jnp.float32) for z in near]
    for n, value in enumerate(rest):
        keep(X_CH + n, value)


def stage_orders(n_columns):
    bits = n_columns.bit_length() - 1
    rest = list(range(1, bits))
    first = [0] if bits else []
    return [first + rest, first + rest[::-1]]


def fused_kernel(
    capacity, n_slabs, n_columns, table_ref, off_ref, frac_ref, norm_ref, weight_ref, out_ref,
    chan, left_a, left_b, third_a, third_b, val_a, val_b, der_a, der_b, grid, done, z_main, z_low, z_high,
    send_sem, recv_sem, send_z, recv_z, *stages
):
    tiles, tile_len = off_ref.shape
    orders = stage_orders(n_columns)
    steps = len(orders[0])
    starts = stages[:2]
    got = (stages[2 : 2 + steps], stages[2 + steps : 2 + 2 * steps])
    sums = (stages[2 + 2 * steps : 1 + 3 * steps], stages[1 + 3 * steps : 4 * steps])
    me_x, me_y = lax.axis_index("gx"), lax.axis_index("yz")
    bufs = ((left_a, third_a, val_a, der_a), (left_b, third_b, val_b, der_b))

    def slab_of(step):
        return lax.rem(me_x + 1 + step, n_slabs)

    def bit_of(k):
        return lax.rem(me_y // (1 << k), 2)

    def partner(k):
        return (me_x, me_y + (1 - 2 * bit_of(k)) * (1 << k))

    barrier = pltpu.get_barrier_semaphore()
    for k in range(steps):
        pl.semaphore_signal(barrier, inc=1, device_id=partner(k), device_id_type=MESH)
    for hop in range(1, n_slabs):
        other = (lax.rem(me_x + hop, n_slabs), me_y)
        pl.semaphore_signal(barrier, inc=1, device_id=other, device_id_type=MESH)

    def prepare_rows(step, _):
        prepare(pl.ds(pl.multiple_of(step * 8, 8), 8), off_ref, frac_ref, norm_ref, weight_ref, chan)
        return 0

    lax.fori_loop(0, tiles // 8, prepare_rows, 0)
    grid[...] = jnp.zeros_like(grid)

    lanes = tile_len
    row_y = lax.broadcasted_iota(jnp.int32, (ROWS_Y, lanes), 0)
    row_y = jnp.where(row_y == ROWS_Y - 1, -1, row_y).astype(jnp.float32)
    row_z = lax.broadcasted_iota(jnp.int32, (PACK, lanes), 0).astype(jnp.float32)
    edge = lax.broadcasted_iota(jnp.int32, (HALO_X, BY, BZ), 1)
    last = n_slabs * n_columns - 1

    def build(g, buf):
        left, third, val, der = buf
        brick = slab_of(g // n_columns) * n_columns + lax.rem(g, n_columns)
        for c in range(capacity):
            entry = table_ref[brick * capacity + c]
            away = jnp.where(entry >= 0, 0.0, 1.0) * (4.0 * BY)
            tile = jnp.maximum(entry, 0)
            for part in range(tile_len // lanes):
                cols = pl.ds(c * tile_len + part * lanes, lanes)

                def row(n):
                    return chan[n, part, pl.ds(tile, 1), :]

                gap = row_y - (row(X_CH) + away)
                hit = [gap == k - 1.0 for k in range(3)]
                wy = pick(hit, [jnp.broadcast_to(row(X_CH + 1 + k), gap.shape) for k in range(3)])
                gy = pick(hit, [jnp.broadcast_to(row(X_CH + 4 + k), gap.shape) for k in range(3)])
                for i in range(HALO_X):
                    band = pl.ds(i * ROWS_Y, ROWS_Y)
                    low = pl.ds((HALO_X + i) * ROWS_Y, ROWS_Y)
                    left[band, cols] = (row(4 * i) * wy + row(4 * i + 1) * gy).astype(jnp.bfloat16)
                    third[band, cols] = (row(4 * i + 2) * wy).astype(jnp.bfloat16)
                    left[low, cols] = (row(4 * i + 3) * wy).astype(jnp.bfloat16)
                hit = [row_z == row(X_CH + 13 + k) for k in range(3)]

                def spread(n, other):
                    for k in range(3):
                        other = jnp.where(hit[k], jnp.broadcast_to(row(X_CH + n + k), row_z.shape), other)
                    return other.astype(jnp.bfloat16)

                value = spread(7, jnp.zeros_like(row_z))
                slope = spread(10, jnp.zeros_like(row_z))
                home = spread(16, jnp.full_like(row_z, -1.0))
                zero = jnp.zeros_like(value)
                for group in range(BZ // PACK):
                    rows = pl.ds(group * PACK, PACK)
                    here = home == jnp.bfloat16(group)
                    val[rows, cols] = jnp.where(here, value, zero)
                    der[rows, cols] = jnp.where(here, slope, zero)

    def multiply(g, buf):
        left, third, val, der = buf
        dims = (((1,), (1,)), ((), ()))
        both = lax.dot_general(left[...], val[...], dims, preferred_element_type=jnp.float32)
        part = lax.dot_general(third[...], der[...], dims, preferred_element_type=jnp.float32)
        half = HALO_X * ROWS_Y
        column = lax.rem(g, n_columns)
        above = jnp.where(column == n_columns - 1, n_columns, column + 1)
        below = jnp.where(column == 0, n_columns, column - 1)
        for f, field in enumerate((both[:half] + part, both[half:])):
            field = field.reshape(HALO_X, ROWS_Y, BZ)
            inner, outer = field[:, :BY], field[:, BY:]
            grid[f, column] += inner
            grid[f, above] += jnp.where(edge == 0, outer, 0.0)
            grid[f, below] += jnp.where(edge == BY - 1, outer, 0.0)

    def stage_refs(f, s, j):
        ref = (starts[f] if s == 0 else sums[f][s - 1]).at[j]
        alive = [k for k in reversed(range(steps)) if k not in orders[f][:s]]
        k = orders[f][s]
        lead = (slice(None),) * alive.index(k)
        return ref, lead, k

    def stage_copy(f, s, j):
        ref, lead, k = stage_refs(f, s, j)
        return pltpu.make_async_remote_copy(
            src_ref=ref.at[lead + (1 - bit_of(k),)],
            dst_ref=got[f][s].at[j],
            send_sem=send_sem.at[f, s, j],
            recv_sem=recv_sem.at[f, s, j],
            device_id=partner(k),
            device_id_type=MESH,
        )

    def cross_copy(kind, j):
        source = (done.at[j, :, pl.ds(1, BX)], done.at[j, :, pl.ds(0, 1)], done.at[j, :, pl.ds(BX + 1, 1)])[kind]
        target = (z_main, z_low, z_high)[kind].at[j]
        owner = lax.rem(me_x + (1, n_slabs, 2)[kind] + j, n_slabs)
        return pltpu.make_async_remote_copy(
            src_ref=source,
            dst_ref=target,
            send_sem=send_z.at[kind, j],
            recv_sem=recv_z.at[kind, j],
            device_id=(owner, me_y),
            device_id_type=MESH,
        )

    at_home = (n_slabs - 1, 0, n_slabs - 2)

    def cross_start(kind, j):
        if isinstance(j, int):
            if j != at_home[kind]:
                cross_copy(kind, j).start()
        else:
            @pl.when(j != at_home[kind])
            def _():
                cross_copy(kind, j).start()

    def event(s, j):
        for f in range(2):
            stage_copy(f, s - 1, j).wait()
            ref, lead, k = stage_refs(f, s - 1, j)
            total = ref[lead + (bit_of(k),)] + got[f][s - 1][j]
            if s == steps:
                done[j, f] = total
            else:
                sums[f][s - 1][j] = total
                stage_copy(f, s, j).start()
        if s == steps:
            for kind in range(3):
                cross_start(kind, j)

    build(0, bufs[0])
    pl.semaphore_wait(barrier, steps + n_slabs - 1)
    pairs = n_columns // 4

    def half_step(h, _):
        step, half = h // 2, lax.rem(h, 2)

        def pair(p, _):
            g = (h * pairs + p) * 2
            build(g + 1, bufs[1])
            multiply(g, bufs[0])
            build(jnp.minimum(g + 2, last), bufs[0])
            multiply(g + 1, bufs[1])
            return 0

        lax.fori_loop(0, pairs, pair, 0)

        @pl.when(half == 1)
        def _():
            for f in range(2):
                for column in range(n_columns):
                    bits = tuple((column >> k) & 1 for k in reversed(range(steps)))
                    starts[f][(step,) + bits] = grid[f, column]
                stage_copy(f, 0, step).start()
            grid[...] = jnp.zeros_like(grid)

        for s in range(1, steps + 1):
            @pl.when((half == (0 if s == 1 else 1)) & (step >= s))
            def _():
                event(s, step - s)

        return 0

    lax.fori_loop(0, 2 * n_slabs, half_step, 0)
    for r in range(1, steps + 1):
        for s in range(r, steps + 1):
            if n_slabs - 1 - (s - r) >= 0:
                event(s, n_slabs - 1 - (s - r))

    main = [done[n_slabs - 1, f, pl.ds(1, BX)] for f in range(2)]
    low = [done[0, f, 0] for f in range(2)]
    high = [done[n_slabs - 2, f, BX + 1] for f in range(2)]
    for j in range(n_slabs):
        for kind in range(3):
            if j != at_home[kind]:
                cross_copy(kind, j).wait()
                for f in range(2):
                    if kind == 0:
                        main[f] = main[f] + z_main[j, f]
                    elif kind == 1:
                        low[f] = low[f] + z_low[j, f, 0]
                    else:
                        high[f] = high[f] + z_high[j, f, 0]
    for f in range(2):
        out = out_ref.at[f]
        out[...] = main[f]
        out[BX - 1] += jnp.where(me_x < n_slabs - 1, low[f], 0.0)
        out[0] += jnp.where(me_x > 0, high[f], 0.0)


def fused(capacity, n_slabs, n_columns, table, off, frac, norm, weight):
    tiles, tile_len = off.shape
    points = capacity * tile_len
    lanes = tile_len
    steps = n_columns.bit_length() - 1
    block = (HALO_X, BY, BZ)
    vmem = pl.BlockSpec(memory_space=pltpu.VMEM)
    smem = pl.BlockSpec(memory_space=pltpu.SMEM)

    def stage(s):
        return pltpu.VMEM((n_slabs,) + (2,) * (steps - s) + block, jnp.float32)

    got = [stage(s + 1) for s in range(steps)]
    sums = [stage(s + 1) for s in range(steps - 1)]
    return pl.pallas_call(
        functools.partial(fused_kernel, capacity, n_slabs, n_columns),
        out_shape=jax.ShapeDtypeStruct((2, BX, BY, BZ), jnp.float32),
        in_specs=[smem, vmem, vmem, vmem, vmem],
        out_specs=vmem,
        scratch_shapes=[pltpu.VMEM((CHANNELS, tile_len // lanes, tiles, lanes), jnp.float32)]
        + [pltpu.VMEM((2 * HALO_X * ROWS_Y, points), jnp.bfloat16)] * 2
        + [pltpu.VMEM((HALO_X * ROWS_Y, points), jnp.bfloat16)] * 2
        + [pltpu.VMEM((BZ, points), jnp.bfloat16)] * 4
        + [
            pltpu.VMEM((2, n_columns + 1) + block, jnp.float32),
            pltpu.VMEM((n_slabs, 2) + block, jnp.float32),
            pltpu.VMEM((n_slabs, 2, BX, BY, BZ), jnp.float32),
            pltpu.VMEM((n_slabs, 2, 1, BY, BZ), jnp.float32),
            pltpu.VMEM((n_slabs, 2, 1, BY, BZ), jnp.float32),
            pltpu.SemaphoreType.DMA((2, steps, n_slabs)),
            pltpu.SemaphoreType.DMA((2, steps, n_slabs)),
            pltpu.SemaphoreType.DMA((3, n_slabs)),
            pltpu.SemaphoreType.DMA((3, n_slabs)),
        ]
        + [stage(0)] * 2 + got * 2 + sums * 2,
        compiler_params=pltpu.CompilerParams(collective_id=0, has_side_effects=True),
        name="fused",
    )(table, off, frac, norm, weight)


def brick_table(capacity, bricks, dest, count):
    tiles = dest.shape[0]
    order = jnp.arange(tiles, dtype=jnp.int32)
    valid = order < count
    earlier = (dest[:, None] == dest[None, :]) & valid[None, :] & (order[None, :] < order[:, None])
    rank = jnp.sum(earlier.astype(jnp.int32), axis=1)
    slot = jnp.where(valid, dest * capacity + rank, -1)
    slots = jnp.arange(bricks * capacity, dtype=jnp.int32)
    found = jnp.where(slots[:, None] == slot[None, :], order[None, :], -1)
    return jnp.max(found, axis=1)


def shards(brick_ids, voxel_offset, fractions, normals, point_weight, tile_count):
    n_slabs = lax.axis_size("gx")
    n_columns = lax.axis_size("yz")
    devices = n_slabs * n_columns
    tiles_here = brick_ids.shape[0]
    capacity = max(2, (tiles_here + devices - 1) // devices)
    table = brick_table(capacity, devices, brick_ids.reshape(tiles_here), tile_count[0])
    both = fused(
        capacity, n_slabs, n_columns, table, voxel_offset,
        jnp.transpose(fractions, (1, 0, 2)), jnp.transpose(normals, (1, 0, 2)), point_weight,
    )
    return (both[0], both[1])


def solution(mesh):
    return jax.shard_map(
        shards,
        mesh=mesh,
        in_specs=(
            P(("gx", "yz"), None),
            P(("gx", "yz"), None),
            P(("gx", "yz"), None, None),
            P(("gx", "yz"), None, None),
            P(("gx", "yz"), None),
            P(("gx", "yz")),
        ),
        out_specs=(P("gx", "yz", None), P("gx", "yz", None)),
        check_vma=False,
    )
```
